32 devices in a mesh: beam: 4 (over y, x), row: 4 (over z), col: 2 (over core).
Axes of the slice: x: 2, y: 2, z: 4, core: 2. Of those that a mesh axis runs over, the one named last changes fastest.
Arguments:
- phase_volume: bfloat16 [64, 1024, 256], P('beam', 'row', 'col'), may hold values from -0.75 to 0.75
- absorb_volume: bfloat16 [64, 1024, 256], P('beam', 'row', 'col'), may hold values from -0.375 to 0.375
- probe: float32 [2, 256, 256], replicated, may hold values from -6 to 6
- amplitudes: bfloat16 [4, 2, 32, 256, 256], P('row', 'col', 'beam'), may hold values from 0.19921875 to 2.5
- scan_rows: int32 [4, 2, 32], P('row', 'col', 'beam'), may hold values from 0 to 255
- scan_cols: int32 [4, 2, 32], P('row', 'col', 'beam'), may hold values from 0 to 127
Outputs:
- object_step: float32 [2, 1024, 256], P(None, 'row', 'col')
- probe_gradient: float32 [2, 256, 256], replicated
- loss: float32 [], replicated
The draws below stay inside these ranges and needn't reach their ends.
All inputs are finite; a program needn't handle non-finite values.
Results may differ from the reference program's by a relative error of at most 0.00055.
The reference program's roundings to bfloat16 on the way count: a program that leaves them out, or rounds other values in their place, can miss the bound.
Values sent between devices are 32-bit elements; how exact they have to be, the bound alone decides.
A program may use at most 64 MiB of HBM per device.

```python
import math
import jax
import jax.numpy as jnp
from jax import lax

ROW_DEV = 256
COL_DEV = 128
PROBE = 256
DEPTH = 64
NROWS = 1024
NCOLS = 256
SCANS = 32
N_ROW = 4
N_COL = 2


def touch_ends(result, stream_key, least, largest):
    longest = result.shape.index(max(result.shape))
    spots = []
    for shift in (0, 1):
        where = [jax.random.randint(jax.random.fold_in(stream_key, axis), (), 0, length) for axis, length in enumerate(result.shape)]
        where[longest] = (where[longest] + shift) % result.shape[longest]
        spots.append(tuple(where))
    return result.at[spots[0]].set(least).at[spots[1]].set(largest)


def block_levels(rng, extent, split, least, largest):
    def one(dim, blocks):
        steps = jax.random.uniform(jax.random.fold_in(jax.random.fold_in(rng, 6), dim), (blocks,), jnp.float32, least / len(split), largest / len(split))
        return jnp.repeat(jnp.exp(steps), extent[dim] // blocks).reshape((-1,) + (1,) * (len(extent) - dim - 1))

    loudness = one(*split[0])
    for cut in split[1:]:
        loudness = loudness * one(*cut)
    return loudness


def normal_values(own_key, shape, scale, most, cuts=(), kind=jnp.bfloat16):
    loudness = block_levels(own_key, shape, cuts, -0.22, 0.18) if cuts else 1.0
    values = jax.random.normal(own_key, shape, jnp.float32) * scale * loudness
    return jnp.minimum(jnp.maximum(values, -most), most).astype(kind)


def setup_inputs(seed: int = 0) -> dict:
    seeds = jax.random.split(jax.random.key(seed), 7)
    return {
        "phase_volume": normal_values(seeds[0], (DEPTH, NROWS, NCOLS), DEPTH ** -0.5, 0.75, ((0, 4), (1, 4), (2, 2))),
        "absorb_volume": normal_values(seeds[1], (DEPTH, NROWS, NCOLS), (4 * DEPTH) ** -0.5, 0.375, ((0, 4), (1, 4), (2, 2))),
        "probe": normal_values(seeds[2], (2, PROBE, PROBE), 1.0, 6.0, (), jnp.float32),
        "amplitudes": jnp.clip(0.19921875 + 2.3007812 * jax.random.uniform(seeds[3], (N_ROW, N_COL, SCANS, PROBE, PROBE), jnp.float32) ** block_levels(seeds[3], (N_ROW, N_COL, SCANS, PROBE, PROBE), ((0, 4), (1, 2), (2, 4)), -0.2, 0.2), 0.19921875, 2.5).astype(jnp.bfloat16),
        "scan_rows": touch_ends(jax.random.randint(seeds[4], (N_ROW, N_COL, SCANS), 0, ROW_DEV), jax.random.fold_in(seeds[4], 1), 0, ROW_DEV - 1).astype(jnp.int32),
        "scan_cols": touch_ends(jax.random.randint(seeds[5], (N_ROW, N_COL, SCANS), 0, COL_DEV), jax.random.fold_in(seeds[5], 1), 0, COL_DEV - 1).astype(jnp.int32),
    }


def dft_tables(length):
    indices = jnp.arange(length, dtype=jnp.int32)
    product = indices[:, None] * indices[None, :] % length
    angles = product.astype(jnp.float32) * (2.0 * math.pi / length)
    factor = 1.0 / math.sqrt(length)
    return ((jnp.cos(angles) * factor).astype(jnp.bfloat16), (-jnp.sin(angles) * factor).astype(jnp.bfloat16))

def left_apply(matrix, batch):
    return jnp.einsum('ab,sbc->sac', matrix.astype(jnp.float32), batch.astype(jnp.float32))

def right_apply(batch, matrix):
    return jnp.einsum('sab,bc->sac', batch.astype(jnp.float32), matrix.astype(jnp.float32))

def window_terms(windows, probe, amplitude, table_real, table_imag):
    phase = windows[:, 0]
    absorb = windows[:, 1]
    damping = jnp.exp(-absorb)
    trans_real = damping * jnp.cos(phase)
    trans_imag = damping * jnp.sin(phase)
    wave_real = probe[0] * trans_real - probe[1] * trans_imag
    wave_imag = probe[0] * trans_imag + probe[1] * trans_real
    send_real = wave_real.astype(jnp.bfloat16)
    send_imag = wave_imag.astype(jnp.bfloat16)
    half_real = (left_apply(table_real, send_real) - left_apply(table_imag, send_imag)).astype(jnp.bfloat16)
    half_imag = (left_apply(table_real, send_imag) + left_apply(table_imag, send_real)).astype(jnp.bfloat16)
    far_real = right_apply(half_real, table_real) - right_apply(half_imag, table_imag)
    far_imag = right_apply(half_real, table_imag) + right_apply(half_imag, table_real)
    modulus = jnp.sqrt(far_real * far_real + far_imag * far_imag)
    misfit = jnp.sum((modulus - amplitude) * (modulus - amplitude))
    ratio = 1.0 - amplitude / jnp.maximum(modulus, 0.5)
    resid_real = (far_real * ratio).astype(jnp.bfloat16)
    resid_imag = (far_imag * ratio).astype(jnp.bfloat16)
    back_real = (left_apply(table_real, resid_real) + left_apply(table_imag, resid_imag)).astype(jnp.bfloat16)
    back_imag = (left_apply(table_real, resid_imag) - left_apply(table_imag, resid_real)).astype(jnp.bfloat16)
    grad_real = right_apply(back_real, table_real) + right_apply(back_imag, table_imag)
    grad_imag = right_apply(back_imag, table_real) - right_apply(back_real, table_imag)
    object_real = wave_real * grad_real + wave_imag * grad_imag
    object_imag = wave_real * grad_imag - wave_imag * grad_real
    cells = jnp.stack([object_imag, -object_real], axis=1)
    probe_real = lax.optimization_barrier(jnp.sum(trans_real * grad_real + trans_imag * grad_imag, axis=0))
    probe_imag = lax.optimization_barrier(jnp.sum(trans_real * grad_imag - trans_imag * grad_real, axis=0))
    return (cells, jnp.stack([probe_real, probe_imag]), misfit)

def reference(phase_volume, absorb_volume, probe, amplitudes, scan_rows, scan_cols):
    half = PROBE // 2
    projection = jnp.stack([lax.optimization_barrier(jnp.sum(phase_volume.astype(jnp.float32), axis=0)), lax.optimization_barrier(jnp.sum(absorb_volume.astype(jnp.float32), axis=0))])
    padded = jnp.pad(projection, ((0, 0), (half, half), (half, half)))
    table_real, table_imag = dft_tables(PROBE)
    tiles = N_ROW * N_COL
    row_list = scan_rows.reshape(tiles, SCANS).astype(jnp.int32)
    col_list = scan_cols.reshape(tiles, SCANS).astype(jnp.int32)
    amp_list = amplitudes.reshape(tiles, SCANS, PROBE, PROBE)
    zero_index = jnp.zeros((), jnp.int32)

    def per_tile(carry, inputs):
        canvas, probe_sum, misfit_sum = carry
        tile, rows_here, cols_here, amp_here = inputs
        row_start = (tile // N_COL * ROW_DEV + rows_here).astype(jnp.int32)
        col_start = (tile % N_COL * COL_DEV + cols_here).astype(jnp.int32)
        windows = jax.vmap(lambda row_at, col_at: lax.dynamic_slice(padded, (zero_index, row_at, col_at), (2, PROBE, PROBE)))(row_start, col_start)
        cells, probe_term, misfit = window_terms(windows, probe, amp_here.astype(jnp.float32), table_real, table_imag)

        def add_window(index, canvas_now):
            where = (zero_index, row_start[index], col_start[index])
            piece = lax.dynamic_slice(canvas_now, where, (2, PROBE, PROBE))
            return lax.dynamic_update_slice(canvas_now, piece + cells[index], where)
        canvas = lax.fori_loop(0, SCANS, add_window, canvas)
        return ((canvas, probe_sum + probe_term, misfit_sum + misfit), None)
    start = (jnp.zeros((2, NROWS + PROBE, NCOLS + PROBE), jnp.float32), jnp.zeros((2, PROBE, PROBE), jnp.float32), jnp.zeros((), jnp.float32))
    inputs = (jnp.arange(tiles, dtype=jnp.int32), row_list, col_list, amp_list)
    (canvas, probe_sum, misfit_sum), _ = lax.scan(per_tile, start, inputs)
    gradient = canvas[:, half:half + NROWS, half:half + NCOLS]
    mean_square = jnp.sum(gradient * gradient) / (2 * NROWS * NCOLS)
    factor = jnp.minimum(1.0, 0.5 / jnp.sqrt(mean_square + 1e-06))
    total = N_ROW * N_COL * SCANS
    return (gradient * factor, probe_sum / total, misfit_sum / (total * PROBE * PROBE))
```

```python
import functools
import math

import jax
import jax.numpy as jnp
import numpy as np
from jax import lax
from jax.experimental import pallas as pl
from jax.experimental.pallas import tpu as pltpu
from jax.sharding import PartitionSpec as P


def from_behind(value, axis, steps):
    count = lax.axis_size(axis)
    first, last = (max(0, -steps), min(count, count - steps))
    return lax.ppermute(value, axis, [(source, source + steps) for source in range(first, last)])


def extended(cells, sides, width):
    for axis, dim in sides:
        count = lax.axis_size(axis)
        ends = count - 1
        head = lax.slice_in_dim(cells, 0, width, axis=dim)
        tail = lax.slice_in_dim(cells, cells.shape[dim] - width, cells.shape[dim], axis=dim)
        cells = jnp.concatenate(
            [
                lax.ppermute(tail, axis, [(i, (i + 1) % count) for i in range(ends)]),
                cells,
                lax.ppermute(head, axis, [((i + 1) % count, i) for i in range(ends)]),
            ],
            axis=dim,
        )
    return cells


def dft_matrices(length):
    indices = np.arange(length, dtype=np.int32)
    product = indices[:, None] * indices[None, :] % length
    angles = product.astype(np.float32) * np.float32(2.0 * math.pi / length)
    factor = np.float32(1.0 / math.sqrt(length))
    real = (np.cos(angles) * factor).astype(jnp.bfloat16)
    imag = (-np.sin(angles) * factor).astype(jnp.bfloat16)
    left = np.block([[real, -imag], [imag, real]])
    right = np.block([[real, imag], [-imag, real]])
    return jnp.asarray(left), jnp.asarray(right)


def fold_rims(canvas, half):
    rows_inner = canvas.shape[1] - 2 * half
    cols_inner = canvas.shape[2] - 2 * half
    middle = canvas[:, :, half : half + cols_inner]
    from_right = from_behind(canvas[:, :, :half], "col", -1)
    from_left = from_behind(canvas[:, :, half + cols_inner :], "col", 1)
    middle = middle + from_right
    middle = middle + from_left
    center = middle[:, half : half + rows_inner, :]
    from_below = from_behind(middle[:, :half, :], "row", -1)
    from_above = from_behind(middle[:, half + rows_inner :, :], "row", 1)
    center = center + jnp.pad(from_below, ((0, 0), (rows_inner - half, 0), (0, 0)))
    return center + jnp.pad(from_above, ((0, 0), (0, rows_inner - half), (0, 0)))


def window_kernel(
    rows_ref, cols_ref, trans_ref, probe_ref, amplitude_ref, left_ref, right_ref,
    canvas_ref, term_ref, misfit_ref,
):
    step = pl.program_id(0)
    length = probe_ref.shape[1]
    wide = trans_ref.shape[2]
    row_at = rows_ref[step]
    col_at = cols_ref[step]

    @pl.when(step == 0)
    def _():
        canvas_ref[...] = jnp.zeros_like(canvas_ref)
        term_ref[...] = jnp.zeros_like(term_ref)
        misfit_ref[...] = jnp.zeros_like(misfit_ref)

    row_base = pl.multiple_of(row_at // 8 * 8, 8)
    row_rest = row_at % 8
    back_by = lax.rem(wide - col_at, wide)

    def window(part):
        rows = trans_ref[part, pl.ds(row_base, length + 8), :]
        rows = pltpu.roll(rows, length + 8 - row_rest, 0)[:length]
        return pltpu.roll(rows, back_by, 1)[:, :length]

    dot = functools.partial(jnp.dot, preferred_element_type=jnp.float32)
    trans_real = window(0)
    trans_imag = window(1)
    wave_real = probe_ref[0] * trans_real - probe_ref[1] * trans_imag
    wave_imag = probe_ref[0] * trans_imag + probe_ref[1] * trans_real
    outgoing = jnp.concatenate([wave_real, wave_imag], axis=0).astype(jnp.bfloat16)
    half = dot(left_ref[...], outgoing).astype(jnp.bfloat16)
    far = dot(jnp.concatenate([half[:length], half[length:]], axis=1), right_ref[...])
    far_real = far[:, :length]
    far_imag = far[:, length:]
    amplitude = amplitude_ref[0].astype(jnp.float32)
    modulus = jnp.sqrt(far_real * far_real + far_imag * far_imag)
    off = modulus - amplitude
    misfit_ref[...] += jnp.sum((off * off).reshape(length // 8, 8, length), axis=0)
    ratio = 1.0 - amplitude / jnp.maximum(modulus, 0.5)
    residual = jnp.concatenate([far_real * ratio, far_imag * ratio], axis=0)
    back = dot(right_ref[...], residual.astype(jnp.bfloat16)).astype(jnp.bfloat16)
    near = dot(jnp.concatenate([back[:length], back[length:]], axis=1), left_ref[...])
    grad_real = near[:, :length]
    grad_imag = near[:, length:]
    trans_real = window(0)
    trans_imag = window(1)
    wave_real = probe_ref[0] * trans_real - probe_ref[1] * trans_imag
    wave_imag = probe_ref[0] * trans_imag + probe_ref[1] * trans_real
    term_ref[0] += trans_real * grad_real + trans_imag * grad_imag
    term_ref[1] += trans_real * grad_imag - trans_imag * grad_real
    side = jnp.zeros((length, wide - length), jnp.float32)
    below = jnp.zeros((8, wide), jnp.float32)

    def spread(part, values):
        placed = pltpu.roll(jnp.concatenate([values, side], axis=1), col_at, 1)
        placed = pltpu.roll(jnp.concatenate([placed, below], axis=0), row_rest, 0)
        canvas_ref[part, pl.ds(row_base, length + 8), :] += placed

    spread(0, wave_real * grad_imag - wave_imag * grad_real)
    spread(1, -(wave_real * grad_real + wave_imag * grad_imag))


def window_terms(trans, probe, amplitude, rows, cols):
    count, length = amplitude.shape[:2]
    left, right = dft_matrices(length)
    whole = lambda array: pl.BlockSpec(array.shape, lambda s, r, c: (0,) * array.ndim)
    outs = [
        jax.ShapeDtypeStruct(trans.shape, jnp.float32),
        jax.ShapeDtypeStruct(probe.shape, jnp.float32),
        jax.ShapeDtypeStruct((8, length), jnp.float32),
    ]
    return pl.pallas_call(
        window_kernel,
        out_shape=outs,
        grid_spec=pltpu.PrefetchScalarGridSpec(
            num_scalar_prefetch=2,
            grid=(count,),
            in_specs=[
                whole(trans),
                whole(probe),
                pl.BlockSpec((1, length, length), lambda s, r, c: (s, 0, 0)),
                whole(left),
                whole(right),
            ],
            out_specs=[whole(out) for out in outs],
        ),
        compiler_params=pltpu.CompilerParams(
            dimension_semantics=("arbitrary",), vmem_limit_bytes=48 * 2**20
        ),
    )(rows, cols, trans, probe, amplitude, left, right)


def local(phase_volume, absorb_volume, probe, amplitudes, scan_rows, scan_cols):
    length = probe.shape[1]
    half = length // 2
    count = scan_rows.shape[2]
    rows_local = phase_volume.shape[1]
    cols_local = phase_volume.shape[2]
    phase_part = jnp.sum(phase_volume, axis=0, dtype=jnp.float32)
    absorb_part = jnp.sum(absorb_volume, axis=0, dtype=jnp.float32)
    phase_sum, absorb_sum = lax.psum((phase_part, absorb_part), "beam")
    padded = extended(jnp.stack([phase_sum, absorb_sum]), (("row", 1), ("col", 2)), half)
    damping = jnp.exp(-padded[1])
    trans = jnp.stack([damping * jnp.cos(padded[0]), damping * jnp.sin(padded[0])])
    canvas, probe_term, misfit = window_terms(
        trans, probe, amplitudes.reshape(count, length, length),
        scan_rows.reshape(count), scan_cols.reshape(count),
    )
    summed, probe_part, misfit_part = lax.psum((canvas, probe_term, jnp.sum(misfit)), "beam")
    probe_total, misfit_total = lax.psum((probe_part, misfit_part), ("row", "col"))
    gradient = fold_rims(summed, half)
    square_sum = lax.psum(jnp.sum(gradient * gradient), ("row", "col"))
    plane_devices = lax.axis_size("row") * lax.axis_size("col")
    mean_square = square_sum / (2 * rows_local * cols_local * plane_devices)
    factor = jnp.minimum(1.0, 0.5 / jnp.sqrt(mean_square + 1e-06))
    total = plane_devices * lax.axis_size("beam") * count
    return (gradient * factor, probe_total / total, misfit_total / (total * length * length))


def solution(mesh):
    in_specs = (
        P("beam", "row", "col"),
        P("beam", "row", "col"),
        P(),
        P("row", "col", "beam", None, None),
        P("row", "col", "beam"),
        P("row", "col", "beam"),
    )
    out_specs = (P(None, "row", "col"), P(), P())
    return jax.shard_map(local, mesh=mesh, in_specs=in_specs, out_specs=out_specs, check_vma=False)
```

```python
import functools
import math

import jax
import jax.numpy as jnp
import numpy as np
from jax import lax
from jax.experimental import pallas as pl
from jax.experimental.pallas import tpu as pltpu
from jax.sharding import PartitionSpec as P


def dft_matrices(length):
    indices = np.arange(length, dtype=np.int32)
    product = indices[:, None] * indices[None, :] % length
    angles = product.astype(np.float32) * np.float32(2.0 * math.pi / length)
    factor = np.float32(1.0 / math.sqrt(length))
    real = (np.cos(angles) * factor).astype(jnp.bfloat16)
    imag = (-np.sin(angles) * factor).astype(jnp.bfloat16)
    left = np.block([[real, -imag], [imag, real]])
    right = np.block([[real, imag], [-imag, real]])
    return jnp.asarray(left), jnp.asarray(right)


def window_kernel(
    rows_ref, cols_ref, trans_ref, probe_ref, amplitude_ref, left_ref, right_ref,
    canvas_ref, term_ref, misfit_ref,
):
    step = pl.program_id(0)
    length = probe_ref.shape[1]
    wide = trans_ref.shape[2]
    row_at = rows_ref[step]
    col_at = cols_ref[step]

    @pl.when(step == 0)
    def _():
        canvas_ref[...] = jnp.zeros_like(canvas_ref)
        term_ref[...] = jnp.zeros_like(term_ref)
        misfit_ref[...] = jnp.zeros_like(misfit_ref)

    row_base = pl.multiple_of(row_at // 8 * 8, 8)
    row_rest = row_at % 8
    back_by = lax.rem(wide - col_at, wide)

    def window(part):
        rows = trans_ref[part, pl.ds(row_base, length + 8), :]
        rows = pltpu.roll(rows, length + 8 - row_rest, 0)[:length]
        return pltpu.roll(rows, back_by, 1)[:, :length]

    dot = functools.partial(jnp.dot, preferred_element_type=jnp.float32)
    trans_real = window(0)
    trans_imag = window(1)
    wave_real = probe_ref[0] * trans_real - probe_ref[1] * trans_imag
    wave_imag = probe_ref[0] * trans_imag + probe_ref[1] * trans_real
    outgoing = jnp.concatenate([wave_real, wave_imag], axis=0).astype(jnp.bfloat16)
    half = dot(left_ref[...], outgoing).astype(jnp.bfloat16)
    far = dot(jnp.concatenate([half[:length], half[length:]], axis=1), right_ref[...])
    far_real = far[:, :length]
    far_imag = far[:, length:]
    amplitude = amplitude_ref[0].astype(jnp.float32)
    modulus = jnp.sqrt(far_real * far_real + far_imag * far_imag)
    off = modulus - amplitude
    misfit_ref[...] += jnp.sum((off * off).reshape(length // 8, 8, length), axis=0)
    ratio = 1.0 - amplitude / jnp.maximum(modulus, 0.5)
    residual = jnp.concatenate([far_real * ratio, far_imag * ratio], axis=0)
    back = dot(right_ref[...], residual.astype(jnp.bfloat16)).astype(jnp.bfloat16)
    near = dot(jnp.concatenate([back[:length], back[length:]], axis=1), left_ref[...])
    grad_real = near[:, :length]
    grad_imag = near[:, length:]
    trans_real = window(0)
    trans_imag = window(1)
    wave_real = probe_ref[0] * trans_real - probe_ref[1] * trans_imag
    wave_imag = probe_ref[0] * trans_imag + probe_ref[1] * trans_real
    term_ref[0] += trans_real * grad_real + trans_imag * grad_imag
    term_ref[1] += trans_real * grad_imag - trans_imag * grad_real
    side = jnp.zeros((length, wide - length), jnp.float32)
    below = jnp.zeros((8, wide), jnp.float32)

    def spread(part, values):
        placed = pltpu.roll(jnp.concatenate([values, side], axis=1), col_at, 1)
        placed = pltpu.roll(jnp.concatenate([placed, below], axis=0), row_rest, 0)
        canvas_ref[part, pl.ds(row_base, length + 8), :] += placed

    spread(0, wave_real * grad_imag - wave_imag * grad_real)
    spread(1, -(wave_real * grad_real + wave_imag * grad_imag))


def window_terms(trans, probe, amplitude, rows, cols):
    count, length = amplitude.shape[:2]
    left, right = dft_matrices(length)
    whole = lambda array: pl.BlockSpec(array.shape, lambda s, r, c: (0,) * array.ndim)
    outs = [
        jax.ShapeDtypeStruct(trans.shape, jnp.float32),
        jax.ShapeDtypeStruct(probe.shape, jnp.float32),
        jax.ShapeDtypeStruct((8, length), jnp.float32),
    ]
    return pl.pallas_call(
        window_kernel,
        out_shape=outs,
        grid_spec=pltpu.PrefetchScalarGridSpec(
            num_scalar_prefetch=2,
            grid=(count,),
            in_specs=[
                whole(trans),
                whole(probe),
                pl.BlockSpec((1, length, length), lambda s, r, c: (s, 0, 0)),
                whole(left),
                whole(right),
            ],
            out_specs=[whole(out) for out in outs],
        ),
        compiler_params=pltpu.CompilerParams(
            dimension_semantics=("arbitrary",), vmem_limit_bytes=48 * 2**20
        ),
    )(rows, cols, trans, probe, amplitude, left, right)


class Sends:
    def __init__(self, axes, send_sem, recv_sem):
        self.axes, self.sends, self.recvs, self.used = axes, send_sem, recv_sem, 0

    def greet(self):
        barrier = pltpu.get_barrier_semaphore()
        peers = 0
        for axis, (me, count) in self.axes.items():
            for d in range(1, count):
                pl.semaphore_signal(
                    barrier, inc=1, device_id={axis: lax.rem(me + d, count)},
                    device_id_type=pl.DeviceIdType.MESH,
                )
                peers += 1
        pl.semaphore_wait(barrier, peers)

    def copy(self, axis, peer, src, dst):
        index = self.used
        self.used += 1
        return pltpu.make_async_remote_copy(
            src_ref=src, dst_ref=dst, send_sem=self.sends.at[index],
            recv_sem=self.recvs.at[index], device_id={axis: peer},
            device_id_type=pl.DeviceIdType.MESH,
        )

    def each(self, axis, source, target):
        me, count = self.axes[axis]
        copies = []
        for d in range(1, count):
            peer = lax.rem(me + d, count)
            one = self.copy(axis, peer, source(peer), target(d - 1))
            one.start()
            copies.append(one)
        return copies

    def sides(self, axis, down, up):
        me, count = self.axes[axis]
        before = self.copy(axis, lax.rem(me + count - 1, count), *down)
        after = self.copy(axis, lax.rem(me + 1, count), *up)
        pl.when(me > 0)(before.start)
        pl.when(me < count - 1)(after.start)

        def finish():
            pl.when(me > 0)(before.wait_send)
            pl.when(me < count - 1)(after.wait_send)
            pl.when(me < count - 1)(before.wait_recv)
            pl.when(me > 0)(after.wait_recv)

        return finish


def wait_all(copies):
    for one in copies:
        one.wait()


def axes_of(sizes):
    return {axis: (lax.axis_index(axis), count) for axis, count in sizes}


def project_kernel(sizes, half, phase_ref, absorb_ref, out_ref, part, slots, piece, tile, strip, side, send_sem, recv_sem):
    axes = axes_of(sizes)
    net = Sends(axes, send_sem, recv_sem)
    beam, beams = axes["beam"]
    row, rows_count = axes["row"]
    col, cols_count = axes["col"]
    depth, rows, cols = phase_ref.shape
    share = rows // beams
    strip[0] = jnp.ones(strip.shape[1:], jnp.float32)
    strip[1] = jnp.zeros(strip.shape[1:], jnp.float32)
    side[:, 0] = jnp.ones((2,) + strip.shape[1:], jnp.float32)
    side[:, 1] = jnp.zeros((2,) + strip.shape[1:], jnp.float32)
    net.greet()
    for plane, ref in enumerate((phase_ref, absorb_ref)):
        total = ref[0].astype(jnp.float32)
        for d in range(1, depth):
            total += ref[d].astype(jnp.float32)
        part[:, plane] = total.reshape(beams, share, cols)
    scatter = net.each("beam", lambda peer: part.at[peer], lambda d: slots.at[d])
    wait_all(scatter)
    total = part[beam]
    for d in range(beams - 1):
        total += slots[d]
    damping = jnp.exp(-total[1])
    piece[0] = damping * jnp.cos(total[0])
    piece[1] = damping * jnp.sin(total[0])
    tile[beam] = piece[...]
    gather = net.each("beam", lambda peer: piece, lambda d: tile.at[beam])
    wait_all(gather)
    for q in range(beams):
        strip[:, half + q * share : half + (q + 1) * share] = tile[q]
    finish = net.sides(
        "row",
        (strip.at[:, pl.ds(half, half)], strip.at[:, pl.ds(half + rows, half)]),
        (strip.at[:, pl.ds(rows, half)], strip.at[:, pl.ds(0, half)]),
    )
    finish()
    finish = net.sides("col", (strip, side.at[1]), (strip, side.at[0]))
    out_ref[:, :, half : half + cols] = strip[...]
    finish()
    out_ref[:, :, :half] = side[0][:, :, cols - half :]
    out_ref[:, :, half + cols :] = side[1][:, :, :half]


def comm_params(number):
    return pltpu.CompilerParams(
        collective_id=number, has_side_effects=True, vmem_limit_bytes=48 * 2**20
    )


def vmem_specs(count):
    return [pl.BlockSpec(memory_space=pltpu.VMEM)] * count


def project(sizes, half, phase_volume, absorb_volume):
    depth, rows, cols = phase_volume.shape
    beams = dict(sizes)["beam"]
    share = rows // beams
    f32 = jnp.float32
    wires = sum(count for _, count in sizes) * 2
    tall = rows + 2 * half
    return pl.pallas_call(
        functools.partial(project_kernel, sizes, half),
        out_shape=jax.ShapeDtypeStruct((2, tall, cols + 2 * half), f32),
        in_specs=vmem_specs(2),
        out_specs=vmem_specs(1)[0],
        scratch_shapes=[
            pltpu.VMEM((beams, 2, share, cols), f32),
            pltpu.VMEM((beams - 1, 2, share, cols), f32),
            pltpu.VMEM((2, share, cols), f32),
            pltpu.VMEM((beams, 2, share, cols), f32),
            pltpu.VMEM((2, tall, cols), f32),
            pltpu.VMEM((2, 2, tall, cols), f32),
            pltpu.SemaphoreType.DMA((wires,)),
            pltpu.SemaphoreType.DMA((wires,)),
        ],
        compiler_params=comm_params(1),
    )(phase_volume, absorb_volume)


def combine_kernel(
    sizes, half, entries, positions, canvas_ref, term_ref, misfit_ref,
    step_ref, probe_ref, loss_ref,
    left, right, side, strip, strip_in, folded, rims, mine, grads,
    term_col, term_a, term_beam, term_b, term_row, result, small, small_sum,
    send_sem, recv_sem,
):
    axes = axes_of(sizes)
    net = Sends(axes, send_sem, recv_sem)
    beam, beams = axes["beam"]
    row, rows_count = axes["row"]
    col, cols_count = axes["col"]
    blocks = strip.shape[1]
    cols = strip.shape[4]
    rims[...] = jnp.zeros_like(rims)
    net.greet()
    left[...] = canvas_ref[:, :, :half]
    right[...] = canvas_ref[:, :, half + cols :]
    finish = net.sides("col", (left, side.at[1]), (right, side.at[0]))
    term_copies = net.each("col", lambda peer: term_ref.at[peer], lambda d: term_col.at[d])
    side_zero = jnp.zeros(side.shape[1:], jnp.float32)

    @pl.when(col == 0)
    def _():
        side[0] = side_zero

    @pl.when(col == cols_count - 1)
    def _():
        side[1] = side_zero

    finish()
    folded_now = canvas_ref[:, :, half : half + cols]
    lower = folded_now[:, :, :half] + side[0]
    strip[...] = (lower + side[1]).reshape(strip.shape)
    grid_copies = net.each("beam", lambda peer: strip.at[:, :, peer], lambda d: strip_in.at[d])
    wait_all(term_copies)
    total = term_ref[col]
    for d in range(cols_count - 1):
        total += term_col[d]
    term_a[...] = total
    term_copies = net.each("beam", lambda peer: term_a.at[peer], lambda d: term_beam.at[d])
    wait_all(grid_copies)
    total = strip[:, :, beam]
    for d in range(beams - 1):
        total += strip_in[d]
    folded[...] = total
    finish = net.sides(
        "row",
        (folded.at[:, 0], rims.at[1]),
        (folded.at[:, blocks - 1], rims.at[0]),
    )
    wait_all(term_copies)
    total = term_a[beam]
    for d in range(beams - 1):
        total += term_beam[d]
    term_b[...] = total
    term_copies = net.each("row", lambda peer: term_b.at[peer], lambda d: term_row.at[d])
    finish()
    mine[...] = folded[:, 1 : blocks - 1]
    mine[:, 0] += rims[0]
    mine[:, blocks - 3] += rims[1]
    grad_copies = net.each("beam", lambda peer: mine, lambda d: grads.at[:, :, beam])
    values = mine[...]
    square = jnp.sum((values * values).reshape(-1, 8, cols), axis=0)
    misfit = misfit_ref[...].reshape(8, misfit_ref.shape[1] // cols, cols)
    misfit_sum = misfit_ref[:, :cols]
    for k in range(1, misfit_ref.shape[1] // cols):
        misfit_sum += misfit_ref[:, k * cols : (k + 1) * cols]
    small_sum[0, 0] = square
    small_sum[0, 1] = misfit_sum
    base = 0

    def share_small(axis, level, base):
        count = axes[axis][1]
        return net.each(axis, lambda peer: small_sum.at[level], lambda d: small.at[base + d]), base + count - 1

    def add_small(level, begin, end):
        total = small_sum[level]
        for k in range(begin, end):
            total += small[k]
        small_sum[level + 1] = total

    small_copies, first = share_small("row", 0, 0)
    wait_all(term_copies)
    total = term_b[row]
    for d in range(rows_count - 1):
        total += term_row[d]
    total = total * (1.0 / positions)
    result[col, beam, row] = total
    term_copies = net.each("row", lambda peer: result.at[col, beam, row], lambda d: result.at[col, beam, row])
    wait_all(small_copies)
    add_small(0, 0, first)
    small_copies, second = share_small("beam", 1, first)
    wait_all(term_copies)
    term_copies = net.each("beam", lambda peer: result.at[col, beam], lambda d: result.at[col, beam])
    wait_all(small_copies)
    add_small(1, first, second)
    small_copies, third = share_small("col", 2, second)
    wait_all(grad_copies)
    grads[:, :, beam] = mine[...]
    wait_all(small_copies)
    add_small(2, second, third)
    mean_square = jnp.sum(small_sum[3, 0], keepdims=True) / entries
    factor = jnp.minimum(1.0, 0.5 / jnp.sqrt(mean_square + 1e-06))
    step_ref[...] = grads[...] * factor[None, None, None]
    loss_ref[...] = jnp.broadcast_to(jnp.sum(small_sum[3, 1], keepdims=True), loss_ref.shape)
    wait_all(term_copies)
    term_copies = net.each("col", lambda peer: result.at[col], lambda d: result.at[col])
    wait_all(term_copies)
    probe_ref[...] = result[...]


def combine(sizes, half, rows, cols, positions, canvas, term, misfit):
    counts = dict(sizes)
    beams, rows_count, cols_count = counts["beam"], counts["row"], counts["col"]
    f32 = jnp.float32
    blocks = rows // half + 2
    thin = half // beams
    lines = term.shape[0] * term.shape[1] // (cols_count * beams * rows_count)
    width = term.shape[2]
    pieces = (cols_count, beams, rows_count, lines, width)
    entries = 2 * rows * cols * rows_count * cols_count
    wires = 4 * sum(counts.values())
    tall = canvas.shape[1]
    grid = (2, blocks - 2, beams, thin, cols)
    step, probe_gradient, loss = pl.pallas_call(
        functools.partial(combine_kernel, sizes, half, entries, positions),
        out_shape=[
            jax.ShapeDtypeStruct(grid, f32),
            jax.ShapeDtypeStruct(pieces, f32),
            jax.ShapeDtypeStruct((8, 128), f32),
        ],
        in_specs=vmem_specs(3),
        out_specs=vmem_specs(3),
        scratch_shapes=[
            pltpu.VMEM((2, tall, half), f32),
            pltpu.VMEM((2, tall, half), f32),
            pltpu.VMEM((2, 2, tall, half), f32),
            pltpu.VMEM((2, blocks, beams, thin, cols), f32),
            pltpu.VMEM((beams - 1, 2, blocks, thin, cols), f32),
            pltpu.VMEM((2, blocks, thin, cols), f32),
            pltpu.VMEM((2, 2, thin, cols), f32),
            pltpu.VMEM((2, blocks - 2, thin, cols), f32),
            pltpu.VMEM(grid, f32),
            pltpu.VMEM((cols_count - 1,) + pieces[1:], f32),
            pltpu.VMEM(pieces[1:], f32),
            pltpu.VMEM((beams - 1,) + pieces[2:], f32),
            pltpu.VMEM(pieces[2:], f32),
            pltpu.VMEM((rows_count - 1,) + pieces[3:], f32),
            pltpu.VMEM(pieces, f32),
            pltpu.VMEM((sum(counts.values()), 2, 8, cols), f32),
            pltpu.VMEM((4, 2, 8, cols), f32),
            pltpu.SemaphoreType.DMA((wires,)),
            pltpu.SemaphoreType.DMA((wires,)),
        ],
        compiler_params=comm_params(2),
    )(canvas, term.reshape(pieces), misfit)
    return (
        step.reshape(2, rows, cols),
        probe_gradient.reshape(term.shape),
        loss[0, 0] / (positions * width * width),
    )


def local(phase_volume, absorb_volume, probe, amplitudes, scan_rows, scan_cols):
    length = probe.shape[1]
    half = length // 2
    count = scan_rows.shape[2]
    rows, cols = phase_volume.shape[1:]
    sizes = tuple((axis, lax.axis_size(axis)) for axis in ("beam", "row", "col"))
    trans = project(sizes, half, phase_volume, absorb_volume)
    canvas, term, misfit = window_terms(
        trans, probe, amplitudes.reshape(count, length, length),
        scan_rows.reshape(count), scan_cols.reshape(count),
    )
    positions = count * math.prod(size for _, size in sizes)
    return combine(sizes, half, rows, cols, positions, canvas, term, misfit)


def solution(mesh):
    in_specs = (
        P("beam", "row", "col"),
        P("beam", "row", "col"),
        P(),
        P("row", "col", "beam", None, None),
        P("row", "col", "beam"),
        P("row", "col", "beam"),
    )
    out_specs = (P(None, "row", "col"), P(), P())
    return jax.shard_map(local, mesh=mesh, in_specs=in_specs, out_specs=out_specs, check_vma=False)
```

```python
import functools
import math

import jax
import jax.numpy as jnp
import numpy as np
from jax import lax
from jax.experimental import pallas as pl
from jax.experimental.pallas import tpu as pltpu
from jax.sharding import PartitionSpec as P


def dft_matrices(length):
    indices = np.arange(length, dtype=np.int32)
    product = indices[:, None] * indices[None, :] % length
    angles = product.astype(np.float32) * np.float32(2.0 * math.pi / length)
    factor = np.float32(1.0 / math.sqrt(length))
    real = (np.cos(angles) * factor).astype(jnp.bfloat16)
    imag = (-np.sin(angles) * factor).astype(jnp.bfloat16)
    left = np.block([[real, -imag], [imag, real]])
    right = np.block([[real, imag], [-imag, real]])
    return jnp.asarray(left), jnp.asarray(right)


def window_kernel(
    rows_ref, cols_ref, trans_ref, probe_ref, amplitude_ref, left_ref, right_ref,
    canvas_ref, term_ref, misfit_ref, kept,
):
    step = pl.program_id(0)
    pair = amplitude_ref.shape[0]
    length = probe_ref.shape[1]
    wide = trans_ref.shape[2]
    dot = functools.partial(jnp.dot, preferred_element_type=jnp.float32)

    @pl.when(step == 0)
    def _():
        canvas_ref[...] = jnp.zeros_like(canvas_ref)
        term_ref[...] = jnp.zeros_like(term_ref)
        misfit_ref[...] = jnp.zeros_like(misfit_ref)

    def place(which):
        row_at = rows_ref[step * pair + which]
        col_at = cols_ref[step * pair + which]
        return pl.multiple_of(row_at // 8 * 8, 8), row_at % 8, col_at

    def wave(which):
        trans_real, trans_imag = kept[which, 0], kept[which, 1]
        wave_real = probe_ref[0] * trans_real - probe_ref[1] * trans_imag
        wave_imag = probe_ref[0] * trans_imag + probe_ref[1] * trans_real
        return trans_real, trans_imag, wave_real, wave_imag

    def enter(which):
        row_base, row_rest, col_at = place(which)
        for part in range(2):
            rows = trans_ref[part, pl.ds(row_base, length + 8), :]
            rows = pltpu.roll(rows, length + 8 - row_rest, 0)[:length]
            kept[which, part] = pltpu.roll(rows, lax.rem(wide - col_at, wide), 1)[:, :length]
        _, _, wave_real, wave_imag = wave(which)
        return jnp.concatenate([wave_real, wave_imag], axis=0).astype(jnp.bfloat16)

    def transform(first, second, values):
        part = dot(first[...], values).astype(jnp.bfloat16)
        return dot(jnp.concatenate([part[:length], part[length:]], axis=1), second[...])

    def compare(which, far):
        far_real = far[:, :length]
        far_imag = far[:, length:]
        amplitude = amplitude_ref[which].astype(jnp.float32)
        modulus = jnp.sqrt(far_real * far_real + far_imag * far_imag)
        off = modulus - amplitude
        misfit_ref[...] += jnp.sum((off * off).reshape(length // 8, 8, length), axis=0)
        ratio = 1.0 - amplitude / jnp.maximum(modulus, 0.5)
        residual = jnp.concatenate([far_real * ratio, far_imag * ratio], axis=0)
        return residual.astype(jnp.bfloat16)

    def leave(which, near):
        row_base, row_rest, col_at = place(which)
        grad_real = near[:, :length]
        grad_imag = near[:, length:]
        trans_real, trans_imag, wave_real, wave_imag = wave(which)
        term_ref[0] += trans_real * grad_real + trans_imag * grad_imag
        term_ref[1] += trans_real * grad_imag - trans_imag * grad_real
        side = jnp.zeros((length, wide - length), jnp.float32)
        below = jnp.zeros((8, wide), jnp.float32)
        object_terms = (
            wave_real * grad_imag - wave_imag * grad_real,
            -(wave_real * grad_real + wave_imag * grad_imag),
        )
        for part, values in enumerate(object_terms):
            placed = pltpu.roll(jnp.concatenate([values, side], axis=1), col_at, 1)
            placed = pltpu.roll(jnp.concatenate([placed, below], axis=0), row_rest, 0)
            canvas_ref[part, pl.ds(row_base, length + 8), :] += placed

    waves = [enter(which) for which in range(pair)]
    fars = [transform(left_ref, right_ref, wave_now) for wave_now in waves]
    residuals = [compare(which, fars[which]) for which in range(pair)]
    nears = [transform(right_ref, left_ref, residual) for residual in residuals]
    for which in range(pair):
        leave(which, nears[which])


def window_terms(trans, probe, amplitude, rows, cols):
    count, length = amplitude.shape[:2]
    pair = 2 if count % 2 == 0 else 1
    left, right = dft_matrices(length)
    whole = lambda array: pl.BlockSpec(array.shape, lambda s, r, c: (0,) * array.ndim)
    outs = [
        jax.ShapeDtypeStruct(trans.shape, jnp.float32),
        jax.ShapeDtypeStruct(probe.shape, jnp.float32),
        jax.ShapeDtypeStruct((8, length), jnp.float32),
    ]
    return pl.pallas_call(
        window_kernel,
        out_shape=outs,
        grid_spec=pltpu.PrefetchScalarGridSpec(
            num_scalar_prefetch=2,
            grid=(count // pair,),
            in_specs=[
                whole(trans),
                whole(probe),
                pl.BlockSpec((pair, length, length), lambda s, r, c: (s, 0, 0)),
                whole(left),
                whole(right),
            ],
            out_specs=[whole(out) for out in outs],
            scratch_shapes=[pltpu.VMEM((pair, 2, length, length), jnp.float32)],
        ),
        compiler_params=pltpu.CompilerParams(
            dimension_semantics=("arbitrary",), vmem_limit_bytes=48 * 2**20
        ),
    )(rows, cols, trans, probe, amplitude, left, right)


class Sends:
    def __init__(self, axes, send_sem, recv_sem):
        self.axes, self.sends, self.recvs, self.used = axes, send_sem, recv_sem, 0

    def greet(self):
        barrier = pltpu.get_barrier_semaphore()
        peers = 0
        for axis, (me, count) in self.axes.items():
            for d in range(1, count):
                pl.semaphore_signal(
                    barrier, inc=1, device_id={axis: lax.rem(me + d, count)},
                    device_id_type=pl.DeviceIdType.MESH,
                )
                peers += 1
        pl.semaphore_wait(barrier, peers)

    def copy(self, axis, peer, src, dst):
        index = self.used
        self.used += 1
        return pltpu.make_async_remote_copy(
            src_ref=src, dst_ref=dst, send_sem=self.sends.at[index],
            recv_sem=self.recvs.at[index], device_id={axis: peer},
            device_id_type=pl.DeviceIdType.MESH,
        )

    def each(self, axis, source, target):
        me, count = self.axes[axis]
        copies = []
        for d in range(1, count):
            peer = lax.rem(me + d, count)
            one = self.copy(axis, peer, source(peer), target(d - 1))
            one.start()
            copies.append(one)
        return copies

    def sides(self, axis, down, up, to_before=True, to_after=True):
        me, count = self.axes[axis]
        before = self.copy(axis, lax.rem(me + count - 1, count), *down)
        after = self.copy(axis, lax.rem(me + 1, count), *up)
        has_before, has_after = me > 0, me < count - 1
        both = jnp.logical_and
        pl.when(both(has_before, to_before))(before.start)
        pl.when(both(has_after, to_after))(after.start)

        def finish():
            pl.when(both(has_before, to_before))(before.wait_send)
            pl.when(both(has_after, to_after))(after.wait_send)
            pl.when(both(has_after, to_before))(before.wait_recv)
            pl.when(both(has_before, to_after))(after.wait_recv)

        return finish


def wait_all(copies):
    for one in copies:
        one.wait()


def axes_of(sizes):
    return {axis: (lax.axis_index(axis), count) for axis, count in sizes}


def project_kernel(sizes, half, phase_ref, absorb_ref, out_ref, part, slots, strip, side, send_sem, recv_sem):
    axes = axes_of(sizes)
    net = Sends(axes, send_sem, recv_sem)
    beam, beams = axes["beam"]
    row, rows_count = axes["row"]
    col, cols_count = axes["col"]
    depth, rows, cols = phase_ref.shape
    share = rows // beams
    edge = half // share
    strip[0] = jnp.ones(strip.shape[1:], jnp.float32)
    strip[1] = jnp.zeros(strip.shape[1:], jnp.float32)
    side[:, 0] = jnp.ones((2,) + strip.shape[1:], jnp.float32)
    side[:, 1] = jnp.zeros((2,) + strip.shape[1:], jnp.float32)
    net.greet()
    for plane, ref in enumerate((phase_ref, absorb_ref)):
        total = ref[0].astype(jnp.float32)
        for d in range(1, depth):
            total += ref[d].astype(jnp.float32)
        part[:, plane] = total.reshape(beams, share, cols)
    scatter = net.each("beam", lambda peer: part.at[peer], lambda d: slots.at[d])
    wait_all(scatter)
    total = part[beam]
    for d in range(beams - 1):
        total += slots[d]
    damping = jnp.exp(-total[1])
    own = edge + beam
    strip[0, own] = damping * jnp.cos(total[0])
    strip[1, own] = damping * jnp.sin(total[0])
    gather = net.each("beam", lambda peer: strip.at[:, own], lambda d: strip.at[:, own])
    finishes = []
    for d in range(beams):
        if d:
            gather[d - 1].wait_recv()
        share_at = lax.rem(beam + beams - d, beams)
        here = strip.at[:, edge + share_at]
        finishes.append(net.sides(
            "row",
            (here, strip.at[:, lax.rem(edge + beams + share_at, strip.shape[1])]),
            (here, strip.at[:, lax.rem(edge + share_at + strip.shape[1] - beams, strip.shape[1])]),
            share_at < edge, share_at >= beams - edge,
        ))
    for one in gather:
        one.wait_send()
    for finish in finishes:
        finish()
    finish = net.sides("col", (strip, side.at[1]), (strip, side.at[0]))
    out_ref[:, :, half : half + cols] = strip[...].reshape(2, rows + 2 * half, cols)
    finish()
    out_ref[:, :, :half] = side[0].reshape(2, rows + 2 * half, cols)[:, :, cols - half :]
    out_ref[:, :, half + cols :] = side[1].reshape(2, rows + 2 * half, cols)[:, :, :half]


def comm_params(number):
    return pltpu.CompilerParams(
        collective_id=number, has_side_effects=True, vmem_limit_bytes=48 * 2**20
    )


def vmem_specs(count):
    return [pl.BlockSpec(memory_space=pltpu.VMEM)] * count


def project(sizes, half, phase_volume, absorb_volume):
    depth, rows, cols = phase_volume.shape
    beams = dict(sizes)["beam"]
    share = rows // beams
    f32 = jnp.float32
    wires = sum(count for _, count in sizes) * 2 + 2 * beams
    tall = rows + 2 * half
    return pl.pallas_call(
        functools.partial(project_kernel, sizes, half),
        out_shape=jax.ShapeDtypeStruct((2, tall, cols + 2 * half), f32),
        in_specs=vmem_specs(2),
        out_specs=vmem_specs(1)[0],
        scratch_shapes=[
            pltpu.VMEM((beams, 2, share, cols), f32),
            pltpu.VMEM((beams - 1, 2, share, cols), f32),
            pltpu.VMEM((2, tall // share, share, cols), f32),
            pltpu.VMEM((2, 2, tall // share, share, cols), f32),
            pltpu.SemaphoreType.DMA((wires,)),
            pltpu.SemaphoreType.DMA((wires,)),
        ],
        compiler_params=comm_params(1),
    )(phase_volume, absorb_volume)


def combine_kernel(
    sizes, half, entries, positions, canvas_ref, term_ref, misfit_ref,
    step_ref, probe_ref, loss_ref,
    left, right, side, strip, strip_in, folded, rims, mine, grads,
    term_col, term_a, term_beam, term_b, term_row, result, small, small_sum,
    send_sem, recv_sem,
):
    axes = axes_of(sizes)
    net = Sends(axes, send_sem, recv_sem)
    beam, beams = axes["beam"]
    row, rows_count = axes["row"]
    col, cols_count = axes["col"]
    blocks = strip.shape[1]
    cols = strip.shape[4]
    rims[...] = jnp.zeros_like(rims)
    net.greet()
    left[...] = canvas_ref[:, :, :half]
    right[...] = canvas_ref[:, :, half + cols :]
    finish = net.sides("col", (left, side.at[1]), (right, side.at[0]))
    term_copies = net.each("col", lambda peer: term_ref.at[peer], lambda d: term_col.at[d])
    side_zero = jnp.zeros(side.shape[1:], jnp.float32)

    @pl.when(col == 0)
    def _():
        side[0] = side_zero

    @pl.when(col == cols_count - 1)
    def _():
        side[1] = side_zero

    finish()
    folded_now = canvas_ref[:, :, half : half + cols]
    lower = folded_now[:, :, :half] + side[0]
    strip[...] = (lower + side[1]).reshape(strip.shape)
    finish = net.sides(
        "row",
        (strip.at[:, 0], rims.at[1]),
        (strip.at[:, blocks - 1], rims.at[0]),
    )
    wait_all(term_copies)
    total = term_ref[col]
    for d in range(cols_count - 1):
        total += term_col[d]
    term_a[...] = total
    term_copies = net.each("beam", lambda peer: term_a.at[peer], lambda d: term_beam.at[d])
    finish()
    folded[...] = strip[:, 1 : blocks - 1]
    folded[:, 0] += rims[0]
    folded[:, blocks - 3] += rims[1]
    grid_copies = net.each("beam", lambda peer: folded.at[:, :, peer], lambda d: strip_in.at[d])
    wait_all(term_copies)
    total = term_a[beam]
    for d in range(beams - 1):
        total += term_beam[d]
    term_b[...] = total
    term_copies = net.each("row", lambda peer: term_b.at[peer], lambda d: term_row.at[d])
    wait_all(grid_copies)
    total = folded[:, :, beam]
    for d in range(beams - 1):
        total += strip_in[d]
    mine[...] = total
    grad_copies = net.each("beam", lambda peer: mine, lambda d: grads.at[:, :, beam])
    values = mine[...]
    square = jnp.sum((values * values).reshape(-1, 8, cols), axis=0)
    misfit_sum = misfit_ref[:, :cols]
    for k in range(1, misfit_ref.shape[1] // cols):
        misfit_sum += misfit_ref[:, k * cols : (k + 1) * cols]
    small_sum[0, 0] = square
    small_sum[0, 1] = misfit_sum
    base = 0

    def share_small(axis, level, base):
        count = axes[axis][1]
        return net.each(axis, lambda peer: small_sum.at[level], lambda d: small.at[base + d]), base + count - 1

    def add_small(level, begin, end):
        total = small_sum[level]
        for k in range(begin, end):
            total += small[k]
        small_sum[level + 1] = total

    small_copies, first = share_small("row", 0, 0)
    wait_all(term_copies)
    total = term_b[row]
    for d in range(rows_count - 1):
        total += term_row[d]
    total = total * (1.0 / positions)
    result[col, beam, row] = total
    term_copies = net.each("row", lambda peer: result.at[col, beam, row], lambda d: result.at[col, beam, row])
    wait_all(small_copies)
    add_small(0, 0, first)
    small_copies, second = share_small("beam", 1, first)
    wait_all(term_copies)
    term_copies = net.each("beam", lambda peer: result.at[col, beam], lambda d: result.at[col, beam])
    wait_all(small_copies)
    add_small(1, first, second)
    small_copies, third = share_small("col", 2, second)
    wait_all(grad_copies)
    grads[:, :, beam] = mine[...]
    wait_all(small_copies)
    add_small(2, second, third)
    mean_square = jnp.sum(small_sum[3, 0], keepdims=True) / entries
    factor = jnp.minimum(1.0, 0.5 / jnp.sqrt(mean_square + 1e-06))
    step_ref[...] = grads[...] * factor[None, None, None]
    loss_ref[...] = jnp.broadcast_to(jnp.sum(small_sum[3, 1], keepdims=True), loss_ref.shape)
    wait_all(term_copies)
    term_copies = net.each("col", lambda peer: result.at[col], lambda d: result.at[col])
    wait_all(term_copies)
    probe_ref[...] = result[...]


def combine(sizes, half, rows, cols, positions, canvas, term, misfit):
    counts = dict(sizes)
    beams, rows_count, cols_count = counts["beam"], counts["row"], counts["col"]
    f32 = jnp.float32
    blocks = rows // half + 2
    thin = half // beams
    lines = term.shape[0] * term.shape[1] // (cols_count * beams * rows_count)
    width = term.shape[2]
    pieces = (cols_count, beams, rows_count, lines, width)
    entries = 2 * rows * cols * rows_count * cols_count
    wires = 4 * sum(counts.values())
    tall = canvas.shape[1]
    grid = (2, blocks - 2, beams, thin, cols)
    step, probe_gradient, loss = pl.pallas_call(
        functools.partial(combine_kernel, sizes, half, entries, positions),
        out_shape=[
            jax.ShapeDtypeStruct(grid, f32),
            jax.ShapeDtypeStruct(pieces, f32),
            jax.ShapeDtypeStruct((8, 128), f32),
        ],
        in_specs=vmem_specs(3),
        out_specs=vmem_specs(3),
        scratch_shapes=[
            pltpu.VMEM((2, tall, half), f32),
            pltpu.VMEM((2, tall, half), f32),
            pltpu.VMEM((2, 2, tall, half), f32),
            pltpu.VMEM((2, blocks, beams, thin, cols), f32),
            pltpu.VMEM((beams - 1, 2, blocks - 2, thin, cols), f32),
            pltpu.VMEM(grid, f32),
            pltpu.VMEM((2, 2, beams, thin, cols), f32),
            pltpu.VMEM((2, blocks - 2, thin, cols), f32),
            pltpu.VMEM(grid, f32),
            pltpu.VMEM((cols_count - 1,) + pieces[1:], f32),
            pltpu.VMEM(pieces[1:], f32),
            pltpu.VMEM((beams - 1,) + pieces[2:], f32),
            pltpu.VMEM(pieces[2:], f32),
            pltpu.VMEM((rows_count - 1,) + pieces[3:], f32),
            pltpu.VMEM(pieces, f32),
            pltpu.VMEM((sum(counts.values()), 2, 8, cols), f32),
            pltpu.VMEM((4, 2, 8, cols), f32),
            pltpu.SemaphoreType.DMA((wires,)),
            pltpu.SemaphoreType.DMA((wires,)),
        ],
        compiler_params=comm_params(2),
    )(canvas, term.reshape(pieces), misfit)
    return (
        step.reshape(2, rows, cols),
        probe_gradient.reshape(term.shape),
        loss[0, 0] / (positions * width * width),
    )


def local(phase_volume, absorb_volume, probe, amplitudes, scan_rows, scan_cols):
    length = probe.shape[1]
    half = length // 2
    count = scan_rows.shape[2]
    rows, cols = phase_volume.shape[1:]
    sizes = tuple((axis, lax.axis_size(axis)) for axis in ("beam", "row", "col"))
    trans = project(sizes, half, phase_volume, absorb_volume)
    canvas, term, misfit = window_terms(
        trans, probe, amplitudes.reshape(count, length, length),
        scan_rows.reshape(count), scan_cols.reshape(count),
    )
    positions = count * math.prod(size for _, size in sizes)
    return combine(sizes, half, rows, cols, positions, canvas, term, misfit)


def solution(mesh):
    in_specs = (
        P("beam", "row", "col"),
        P("beam", "row", "col"),
        P(),
        P("row", "col", "beam", None, None),
        P("row", "col", "beam"),
        P("row", "col", "beam"),
    )
    out_specs = (P(None, "row", "col"), P(), P())
    return jax.shard_map(local, mesh=mesh, in_specs=in_specs, out_specs=out_specs, check_vma=False)
```
